8 devices in a mesh: model: 4 (over z, y, x), data: 2 (over core).
Axes of the slice: x: 2, y: 2, z: 1, core: 2. Of those that a mesh axis runs over, the one named last changes fastest.
Arguments:
- grad_qkv: float32 [2, 12, 512, 1536], P('data', None, None, 'model')
- weight_qkv: float32 [12, 512, 1536], P(None, 'data', 'model')
- moment1_qkv: float32 [12, 512, 1536], P(None, 'data', 'model')
- moment2_qkv: float32 [12, 512, 1536], P(None, 'data', 'model')
- grad_proj: float32 [2, 12, 512, 512], P('data', None, 'model')
- weight_proj: float32 [12, 512, 512], P(None, ('model', 'data'))
- moment1_proj: float32 [12, 512, 512], P(None, ('model', 'data'))
- moment2_proj: float32 [12, 512, 512], P(None, ('model', 'data'))
- grad_fcin: float32 [2, 12, 512, 2048], P('data', None, None, 'model')
- weight_fcin: float32 [12, 512, 2048], P(None, 'data', 'model')
- moment1_fcin: float32 [12, 512, 2048], P(None, 'data', 'model')
- moment2_fcin: float32 [12, 512, 2048], P(None, 'data', 'model')
- grad_fcout: float32 [2, 12, 2048, 512], P('data', None, 'model')
- weight_fcout: float32 [12, 2048, 512], P(None, ('model', 'data'))
- moment1_fcout: float32 [12, 2048, 512], P(None, ('model', 'data'))
- moment2_fcout: float32 [12, 2048, 512], P(None, ('model', 'data'))
Outputs:
- output 1: bfloat16 [12, 512, 1536], P(None, None, 'model')
- output 2: bfloat16 [12, 512, 512], P(None, 'model')
- output 3: bfloat16 [12, 512, 2048], P(None, None, 'model')
- output 4: bfloat16 [12, 2048, 512], P(None, 'model')
- output 5: float32 [12, 512, 1536], P(None, 'data', 'model')
- output 6: float32 [12, 512, 512], P(None, ('model', 'data'))
- output 7: float32 [12, 512, 2048], P(None, 'data', 'model')
- output 8: float32 [12, 2048, 512], P(None, ('model', 'data'))
- output 9: float32 [12, 512, 1536], P(None, 'data', 'model')
- output 10: float32 [12, 512, 512], P(None, ('model', 'data'))
- output 11: float32 [12, 512, 2048], P(None, 'data', 'model')
- output 12: float32 [12, 2048, 512], P(None, ('model', 'data'))
- output 13: float32 [12, 512, 1536], P(None, 'data', 'model')
- output 14: float32 [12, 512, 512], P(None, ('model', 'data'))
- output 15: float32 [12, 512, 2048], P(None, 'data', 'model')
- output 16: float32 [12, 2048, 512], P(None, ('model', 'data'))
All inputs are finite; a program needn't handle non-finite values.
Results may differ from the reference program's by a relative error of at most 0.001.
Values are sent between devices in bfloat16 or wider.
A program may use at most 1 GiB of HBM per device.

```python
import jax
import jax.numpy as jnp

D_MODEL = 512
FF_DIM = 2048
LAYERS = 12
DATA_SIZE = 2
STEP_COUNT = 100

LEARN_RATE = 0.08
BETA_ONE = 0.9
BETA_TWO = 0.999
ADAM_EPS = 1e-6
DECAY_RATE = 0.01
MAX_NORM = 1.0
TILT_RATE = 0.8
KIND_NAMES = ("qkv", "proj", "fcin", "fcout")
KIND_SHAPES = ((D_MODEL, 3 * D_MODEL), (D_MODEL, D_MODEL), (D_MODEL, FF_DIM), (FF_DIM, D_MODEL))


def tilt_profile(num_rows, num_cols):
    row_pos = (jnp.arange(num_rows, dtype=jnp.float32) + 0.5) / num_rows
    col_pos = (jnp.arange(num_cols, dtype=jnp.float32) + 0.5) / num_cols
    row_scale = jnp.exp(TILT_RATE * (2.0 * row_pos - 1.0))
    col_scale = jnp.exp(TILT_RATE * (2.0 * col_pos - 1.0))
    return row_scale[:, None] * col_scale[None, :]


def setup_inputs(seed: int = 0) -> dict:
    base_key = jax.random.key(seed)
    norm_ratio = jax.random.uniform(jax.random.fold_in(base_key, 100), (), jnp.float32, 2.5, 4.5)
    raw_grads = []
    grad_scales = []
    total_sq = jnp.zeros((), jnp.float32)
    for kind_idx, shape_pair in enumerate(KIND_SHAPES):
        num_rows, num_cols = shape_pair
        kind_keys = jax.random.split(jax.random.fold_in(base_key, kind_idx), 7)
        grad_scale = jnp.exp(jax.random.uniform(kind_keys[0], (LAYERS, 1, 1), jnp.float32, -1.1, 1.1))
        common = jax.random.normal(kind_keys[1], (1, LAYERS, num_rows, num_cols), jnp.float32)
        dev_noise = jax.random.normal(kind_keys[2], (DATA_SIZE, LAYERS, num_rows, num_cols), jnp.float32)
        raw_grad = grad_scale * (common + dev_noise)
        mean_grad = jnp.mean(raw_grad, axis=0)
        total_sq = total_sq + jnp.sum(mean_grad * mean_grad)
        raw_grads.append(raw_grad)
        grad_scales.append(grad_scale)
    factor = norm_ratio * MAX_NORM / jnp.sqrt(total_sq)
    inputs = {}
    for kind_idx, shape_pair in enumerate(KIND_SHAPES):
        num_rows, num_cols = shape_pair
        kind_name = KIND_NAMES[kind_idx]
        kind_keys = jax.random.split(jax.random.fold_in(base_key, kind_idx), 7)
        profile = tilt_profile(num_rows, num_cols)
        weight_scale = jnp.exp(jax.random.uniform(kind_keys[3], (LAYERS, 1, 1), jnp.float32, -1.1, 1.1)) * num_rows ** -0.5
        clip_scale = grad_scales[kind_idx] * factor / norm_ratio
        shape_full = (LAYERS, num_rows, num_cols)
        inputs["grad_" + kind_name] = raw_grads[kind_idx] * factor
        inputs["weight_" + kind_name] = jax.random.normal(kind_keys[4], shape_full, jnp.float32) * weight_scale * profile
        inputs["moment1_" + kind_name] = jax.random.normal(kind_keys[5], shape_full, jnp.float32) * clip_scale
        inputs["moment2_" + kind_name] = (clip_scale * profile) ** 2 * jax.random.uniform(kind_keys[6], shape_full, jnp.float32, 0.5, 1.5)
    return inputs


def lamb_tensor(grad_mean, weight, moment1, moment2, clip_coef):
    clipped = clip_coef * grad_mean
    new_first = BETA_ONE * moment1 + (1.0 - BETA_ONE) * clipped
    new_second = BETA_TWO * moment2 + (1.0 - BETA_TWO) * clipped * clipped
    first_hat = new_first / (1.0 - BETA_ONE ** STEP_COUNT)
    second_hat = new_second / (1.0 - BETA_TWO ** STEP_COUNT)
    update = first_hat / (jnp.sqrt(second_hat) + ADAM_EPS) + DECAY_RATE * weight
    weight_norm = jnp.sqrt(jnp.sum(weight * weight, axis=(1, 2), keepdims=True))
    update_norm = jnp.sqrt(jnp.sum(update * update, axis=(1, 2), keepdims=True))
    new_weight = weight - LEARN_RATE * (weight_norm / update_norm) * update
    return new_weight, new_first, new_second


def reference(grad_qkv, weight_qkv, moment1_qkv, moment2_qkv, grad_proj, weight_proj, moment1_proj, moment2_proj, grad_fcin, weight_fcin, moment1_fcin, moment2_fcin, grad_fcout, weight_fcout, moment1_fcout, moment2_fcout):
    grad_list = (grad_qkv, grad_proj, grad_fcin, grad_fcout)
    states = ((weight_qkv, moment1_qkv, moment2_qkv), (weight_proj, moment1_proj, moment2_proj), (weight_fcin, moment1_fcin, moment2_fcin), (weight_fcout, moment1_fcout, moment2_fcout))
    grad_means = [jnp.sum(grad_stack.astype(jnp.bfloat16).astype(jnp.float32), axis=0) / DATA_SIZE for grad_stack in grad_list]
    total_sq = sum(jnp.sum(grad_mean * grad_mean) for grad_mean in grad_means)
    clip_coef = jnp.minimum(1.0, MAX_NORM / jnp.sqrt(total_sq))
    results = [lamb_tensor(grad_means[kind_idx], states[kind_idx][0], states[kind_idx][1], states[kind_idx][2], clip_coef) for kind_idx in range(4)]
    replicas = [outcome[0].astype(jnp.bfloat16) for outcome in results]
    return (replicas[0], replicas[1], replicas[2], replicas[3], results[0][0], results[1][0], results[2][0], results[3][0], results[0][1], results[1][1], results[2][1], results[3][1], results[0][2], results[1][2], results[2][2], results[3][2])
```

```python
import functools

import jax
import jax.numpy as jnp
from jax import lax
from jax.experimental import pallas as pl
from jax.experimental.pallas import tpu as pltpu
from jax.sharding import PartitionSpec as P

LEARN_RATE = 0.08
BETA_ONE = 0.9
BETA_TWO = 0.999
ADAM_EPS = 1e-6
DECAY_RATE = 0.01
MAX_NORM = 1.0
STEP_COUNT = 100
COLUMN_SPLIT = (True, False, True, False)
ORDER = (2, 3, 0, 1)
MESH_ID = pl.DeviceIdType.MESH
SCOPED_BYTES = 25 * 2**19

STAGE_SLOTS = 4
SEND_SLOTS = 4
COMBINE_LAG = 3
STATE_SLOTS = 12
STATE_AHEAD = 6


def grad_spec(col_split):
    return P("data", None, None, "model") if col_split else P("data", None, "model", None)


def state_spec(col_split):
    return P(None, "data", "model") if col_split else P(None, ("model", "data"), None)


def replica_spec(col_split):
    return P(None, None, "model") if col_split else P(None, "model", None)


def at_offset(pos, idx, off, layers, count, action):
    target = idx + off
    if off == 0:
        action(pos, idx)
    elif off > 0:
        pl.when(target < layers)(lambda: action(pos, target))
        if pos + 1 < count:
            pl.when(target >= layers)(lambda: action(pos + 1, target - layers))
    else:
        pl.when(target >= 0)(lambda: action(pos, target))
        if pos > 0:
            pl.when(target < 0)(lambda: action(pos - 1, target + layers))


def fold_lanes(acc):
    return functools.reduce(jnp.add, [acc[:, lo:lo + 128] for lo in range(0, acc.shape[1], 128)])


class Resident:
    def __init__(self, ref, layers, shapes):
        self.ref, self.shapes = ref, shapes
        full = max(rows for rows, _ in shapes)
        self.packed = [full // rows for rows, _ in shapes]
        self.base, total = [], 0
        for packed in self.packed:
            self.base.append(total)
            total += -(-layers // packed)
        self.slots = total

    def spot(self, pos, layer):
        packed = self.packed[pos]
        if packed == 1:
            return self.base[pos] + layer, 0
        rows = self.shapes[pos][0]
        return self.base[pos] + layer // packed, pl.multiple_of(lax.rem(layer, packed) * rows, rows)

    def block(self, which, pos, layer):
        rows, cols = self.shapes[pos]
        slot, row = self.spot(pos, layer)
        return self.ref.at[which, slot, pl.ds(row, rows), pl.ds(0, cols)]


def other_devices(model_size, data_size):
    return [(dm, dd) for dm in range(model_size) for dd in range(data_size) if (dm, dd) != (0, 0)]


class Peers:
    def __init__(self, model_size, data_size):
        self.model_size, self.data_size = model_size, data_size
        self.me_m, self.me_d = lax.axis_index("model"), lax.axis_index("data")
        self.me = self.me_m * data_size + self.me_d
        self.offsets = other_devices(model_size, data_size)

    def there(self, off):
        return lax.rem(self.me_m + off[0], self.model_size), lax.rem(self.me_d + off[1], self.data_size)

    def back(self, off):
        from_m = lax.rem(self.me_m + self.model_size - off[0], self.model_size)
        from_d = lax.rem(self.me_d + self.data_size - off[1], self.data_size)
        return from_m * self.data_size + from_d

    def arrive(self):
        barrier = pltpu.get_barrier_semaphore()
        for off in self.offsets:
            to_m, to_d = self.there(off)
            pl.semaphore_signal(barrier, inc=1, device_id=(to_m, to_d), device_id_type=MESH_ID)

    def await_all(self):
        pl.semaphore_wait(pltpu.get_barrier_semaphore(), len(self.offsets))

    def copies(self, slots, send_sem, recv_sem):
        out = []
        for num, off in enumerate(self.offsets):
            to_m, to_d = self.there(off)
            out.append(pltpu.make_async_remote_copy(
                src_ref=slots.at[self.me], dst_ref=slots.at[self.me], send_sem=send_sem.at[num],
                recv_sem=recv_sem.at[self.me], device_id=(to_m, to_d), device_id_type=MESH_ID))
        return out

    def wait_copies(self, copies, slots, send_sem, recv_sem):
        for num, off in enumerate(self.offsets):
            src = self.back(off)
            copies[num].wait_send()
            to_m, to_d = self.there(off)
            pltpu.make_async_remote_copy(
                src_ref=slots.at[src], dst_ref=slots.at[src], send_sem=send_sem.at[num],
                recv_sem=recv_sem.at[src], device_id=(to_m, to_d), device_id_type=MESH_ID).wait_recv()


def grad_kernel(dims, g0, g1, g2, g3, w0, w1, w2, w3, held_ref, coef_ref,
                r0, r1, r2, r3, stage, outbox, acc_ref, slots, other_sem, own_sem, w_sem, send_sem, recv_sem, tile_send, tile_recv):
    layers, shapes, model_size, data_size = dims
    grads, weights = [(g0, g1, g2, g3)[k] for k in ORDER], [(w0, w1, w2, w3)[k] for k in ORDER]
    inbox, shapes = [(r0, r1, r2, r3)[k] for k in ORDER], [shapes[k] for k in ORDER]
    count = len(ORDER)
    held = Resident(held_ref, layers, shapes)
    peers = Peers(model_size, data_size)
    mine, theirs = peers.me_d, 1 - peers.me_d
    peers.arrive()

    def number(pos, layer):
        return pos * layers + layer

    def rows_of(pos, who):
        return pl.ds(pl.multiple_of(who * shapes[pos][0], shapes[pos][0]), shapes[pos][0])

    def load_other(pos, layer):
        rows, cols = shapes[pos]
        slot = lax.rem(number(pos, layer), STAGE_SLOTS)
        return pltpu.make_async_copy(grads[pos].at[0, layer, rows_of(pos, theirs), :], stage.at[slot, pl.ds(0, rows), pl.ds(0, cols)], other_sem.at[slot])

    def load_own(pos, layer):
        return pltpu.make_async_copy(grads[pos].at[0, layer, rows_of(pos, mine), :], held.block(0, pos, layer), own_sem.at[number(pos, layer)])

    def load_weight(pos, layer):
        return pltpu.make_async_copy(weights[pos].at[layer], held.block(1, pos, layer), w_sem.at[number(pos, layer)])

    def send(pos, layer):
        rows, cols = shapes[pos]
        slot = lax.rem(number(pos, layer), SEND_SLOTS)
        return pltpu.make_async_remote_copy(
            src_ref=outbox.at[slot, pl.ds(0, rows), pl.ds(0, cols)], dst_ref=inbox[pos].at[layer], send_sem=send_sem.at[slot],
            recv_sem=recv_sem.at[number(pos, layer)], device_id=(peers.me_m, theirs), device_id_type=MESH_ID)

    def pack(pos, layer):
        rows, cols = shapes[pos]
        num = number(pos, layer)
        slot, box = lax.rem(num, STAGE_SLOTS), lax.rem(num, SEND_SLOTS)
        load_other(pos, layer).wait()

        def step(t, _):
            at = pl.ds(pl.multiple_of(t * 32, 32), 32)
            outbox[box, at, pl.ds(0, cols)] = stage[slot, at, pl.ds(0, cols)].astype(jnp.bfloat16)
            return 0

        lax.fori_loop(0, rows // 32, step, 0, unroll=2)

    def combine(pos, layer):
        rows, cols = shapes[pos]
        load_own(pos, layer).wait()
        send(pos, layer).wait_recv()
        block, row = held.spot(pos, layer)
        wide = pl.ds(0, cols)

        def step(t, acc):
            at = pl.ds(pl.multiple_of(t * 16, 16), 16)
            there = pl.ds(pl.multiple_of(row + t * 16, 16), 16)
            own = held_ref[0, block, there, wide].astype(jnp.bfloat16).astype(jnp.float32)
            mean = (own + inbox[pos][layer, at, :].astype(jnp.float32)) * (1.0 / data_size)
            held_ref[0, block, there, wide] = mean
            sq = mean * mean
            return acc + sq[:8] + sq[8:]

        acc = lax.fori_loop(0, rows // 16, step, jnp.zeros((8, cols), jnp.float32), unroll=2)
        acc_ref[...] += fold_lanes(acc)

    acc_ref[...] = jnp.zeros_like(acc_ref)
    for layer in range(STAGE_SLOTS):
        load_other(0, layer).start()
        load_own(0, layer).start()
    for layer in range(2):
        load_weight(0, layer).start()
    for pos in range(count):
        def body(layer, _, pos=pos):
            if pos == 0:
                pl.when(layer >= SEND_SLOTS)(lambda: send(pos, layer - SEND_SLOTS).wait_send())
            else:
                at_offset(pos, layer, -SEND_SLOTS, layers, count, lambda p, l: send(p, l).wait_send())
            pack(pos, layer)
            if pos == 0:
                pl.when(layer == 0)(peers.await_all)
            at_offset(pos, layer, -1, layers, count, lambda p, l: send(p, l).start())

            def ahead(p, l):
                load_other(p, l).start()
                load_own(p, l).start()

            at_offset(pos, layer, STAGE_SLOTS, layers, count, ahead)
            at_offset(pos, layer, 2, layers, count, lambda p, l: load_weight(p, l).start())
            at_offset(pos, layer, -COMBINE_LAG, layers, count, combine)
            return 0

        lax.fori_loop(0, layers, body, 0)
    last = count - 1
    send(last, layers - 1).start()
    for layer in range(layers - COMBINE_LAG, layers):
        combine(last, layer)
    for layer in range(layers - SEND_SLOTS, layers):
        send(last, layer).wait_send()

    slots[peers.me] = acc_ref[...]
    copies = peers.copies(slots, tile_send, tile_recv)
    for copy in copies:
        copy.start()
    for pos in range(count):
        def drain(layer, _, pos=pos):
            load_weight(pos, layer).wait()
            return 0

        lax.fori_loop(0, layers, drain, 0)
    peers.wait_copies(copies, slots, tile_send, tile_recv)
    total = functools.reduce(jnp.add, [slots[n] for n in range(model_size * data_size)])
    total = jnp.sum(jnp.sum(total, axis=1, keepdims=True), axis=0, keepdims=True)
    coef_ref[...] = jnp.broadcast_to(jnp.minimum(1.0, MAX_NORM / jnp.sqrt(total)), coef_ref.shape)


def adam_kernel(dims, *refs):
    layers, shapes = dims
    count = len(ORDER)
    coef_ref = refs[0]
    m_in, v_in, held_ref, m_out, v_out = refs[2:6], refs[6:10], refs[10], refs[11:15], refs[15:19]
    usq_ref, wsq_ref, ring, load_sem, store_sem = refs[19:]
    pick = lambda group: [group[k] for k in ORDER]
    m_in, v_in, m_out, v_out, shapes = map(pick, (m_in, v_in, m_out, v_out, shapes))
    held = Resident(held_ref, layers, shapes)
    coef = jnp.max(coef_ref[...])

    def number(pos, layer):
        return pos * layers + layer

    def window(pos, slot, which):
        rows, cols = shapes[pos]
        return ring.at[slot, which, pl.ds(0, rows), pl.ds(0, cols)]

    def loads(pos, layer):
        slot = lax.rem(number(pos, layer), STATE_SLOTS)
        return [pltpu.make_async_copy(src[pos].at[layer], window(pos, slot, which), load_sem.at[slot, which]) for which, src in enumerate((m_in, v_in))]

    def stores(pos, layer):
        slot = lax.rem(number(pos, layer), STATE_SLOTS)
        return [pltpu.make_async_copy(window(pos, slot, which), dst[pos].at[layer], store_sem.at[slot, which]) for which, dst in enumerate((m_out, v_out))]

    def start_loads(pos, layer):
        for copy in loads(pos, layer):
            copy.start()

    def wait_stores(pos, layer):
        for copy in stores(pos, layer):
            copy.wait()

    def compute(pos, layer):
        rows, cols = shapes[pos]
        num = number(pos, layer)
        slot = lax.rem(num, STATE_SLOTS)
        block, row = held.spot(pos, layer)

        def step(t, accs):
            at, wide = pl.ds(pl.multiple_of(t * 8, 8), 8), pl.ds(0, cols)
            there = pl.ds(pl.multiple_of(row + t * 8, 8), 8)
            clipped = coef * held_ref[0, block, there, wide]
            weight = held_ref[1, block, there, wide]
            first = BETA_ONE * ring[slot, 0, at, wide] + (1.0 - BETA_ONE) * clipped
            second = BETA_TWO * ring[slot, 1, at, wide] + (1.0 - BETA_TWO) * clipped * clipped
            ring[slot, 0, at, wide] = first
            ring[slot, 1, at, wide] = second
            first_hat = first * (1.0 / (1.0 - BETA_ONE ** STEP_COUNT))
            second_hat = second * (1.0 / (1.0 - BETA_TWO ** STEP_COUNT))
            update = first_hat / (jnp.sqrt(second_hat) + ADAM_EPS) + DECAY_RATE * weight
            held_ref[0, block, there, wide] = update
            return accs[0] + update * update, accs[1] + weight * weight

        zero = jnp.zeros((8, cols), jnp.float32)
        usq, wsq = lax.fori_loop(0, rows // 8, step, (zero, zero), unroll=2)
        usq_ref[num] = fold_lanes(usq)
        wsq_ref[num] = fold_lanes(wsq)

    for layer in range(STATE_AHEAD):
        start_loads(0, layer)
    for pos in range(count):
        def body(layer, _, pos=pos):
            at_offset(pos, layer, STATE_AHEAD - STATE_SLOTS, layers, count, wait_stores)
            at_offset(pos, layer, STATE_AHEAD, layers, count, start_loads)
            for copy in loads(pos, layer):
                copy.wait()
            compute(pos, layer)
            for copy in stores(pos, layer):
                copy.start()
            return 0

        lax.fori_loop(0, layers, body, 0)
    for layer in range(layers - STATE_SLOTS + STATE_AHEAD, layers):
        wait_stores(count - 1, layer)


def weight_kernel(dims, usq_ref, wsq_ref, _, held_ref, r0, r1, r2, r3, outbox, slots, tile_send, tile_recv, send_sem, recv_sem):
    layers, shapes, model_size, data_size = dims
    count = len(ORDER)
    inbox, shapes = [(r0, r1, r2, r3)[k] for k in ORDER], [shapes[k] for k in ORDER]
    held = Resident(held_ref, layers, shapes)
    peers = Peers(model_size, data_size)
    peers.arrive()

    def number(pos, layer):
        return pos * layers + layer

    def send(pos, layer):
        rows, cols = shapes[pos]
        block, row = held.spot(pos, layer)
        return pltpu.make_async_remote_copy(
            src_ref=outbox.at[block, pl.ds(row, rows), pl.ds(0, cols)], dst_ref=inbox[pos].at[layer], send_sem=send_sem.at[number(pos, layer)],
            recv_sem=recv_sem.at[number(pos, layer)], device_id=(peers.me_m, 1 - peers.me_d), device_id_type=MESH_ID)

    def by_lane(ref):
        part = jnp.sum(ref[...], axis=1)
        part = jnp.concatenate([part, jnp.zeros((128 - part.shape[0], 128), jnp.float32)], axis=0)
        return jnp.sum(part.T, axis=0, keepdims=True)

    row = lax.broadcasted_iota(jnp.int32, (8, 128), 0)
    lane = lax.broadcasted_iota(jnp.int32, (8, 128), 1)
    slots[peers.me] = jnp.where(row == 0, by_lane(usq_ref), by_lane(wsq_ref))
    peers.await_all()
    copies = peers.copies(slots, tile_send, tile_recv)
    for copy in copies:
        copy.start()
    peers.wait_copies(copies, slots, tile_send, tile_recv)
    total = functools.reduce(jnp.add, [slots[n] for n in range(model_size * data_size)])
    root = jnp.sqrt(total)
    live = (row == 1) & (lane < count * layers)
    rates = jnp.where(live, LEARN_RATE * (root / jnp.where(lane < count * layers, root[0:1], 1.0)), 0.0)

    for pos in range(count):
        rows, cols = shapes[pos]

        def body(layer, _, pos=pos, rows=rows, cols=cols):
            num = number(pos, layer)
            rate = jnp.sum(jnp.where(lane == num, rates, 0.0))
            block, row = held.spot(pos, layer)
            wide = pl.ds(0, cols)

            def step(t, _):
                there = pl.ds(pl.multiple_of(row + t * 16, 16), 16)
                new = held_ref[1, block, there, wide] - rate * held_ref[0, block, there, wide]
                held_ref[1, block, there, wide] = new
                outbox[block, there, wide] = new.astype(jnp.bfloat16)
                return 0

            lax.fori_loop(0, rows // 16, step, 0, unroll=2)
            at_offset(pos, layer, -1, layers, count, lambda p, l: send(p, l).start())
            return 0

        lax.fori_loop(0, layers, body, 0)
    send(count - 1, layers - 1).start()
    for pos in range(count):
        def drain(layer, _, pos=pos):
            send(pos, layer).wait()
            return 0

        lax.fori_loop(0, layers, drain, 0)


def write_kernel(dims, held_ref, i0, i1, i2, i3, w0, w1, w2, w3, r0, r1, r2, r3, outbox, weight_sem, inbox_sem, own_sem):
    layers, shapes = dims
    count = len(ORDER)
    pick = lambda group: [group[k] for k in ORDER]
    inbox, weights, replicas, shapes = map(pick, ((i0, i1, i2, i3), (w0, w1, w2, w3), (r0, r1, r2, r3), shapes))
    held = Resident(held_ref, layers, shapes)
    me_d = lax.axis_index("data")

    def rows_of(pos, who):
        return pl.ds(pl.multiple_of(who * shapes[pos][0], shapes[pos][0]), shapes[pos][0])

    def weight_copy(pos, layer):
        return pltpu.make_async_copy(held.block(1, pos, layer), weights[pos].at[layer], weight_sem.at[pos * layers + layer])

    def inbox_copy(pos, layer):
        return pltpu.make_async_copy(inbox[pos].at[layer], replicas[pos].at[layer, rows_of(pos, 1 - me_d), :], inbox_sem.at[pos * layers + layer])

    def own_copy(pos, layer):
        rows, cols = shapes[pos]
        slot = lax.rem(pos * layers + layer, SEND_SLOTS)
        return pltpu.make_async_copy(outbox.at[slot, pl.ds(0, rows), pl.ds(0, cols)], replicas[pos].at[layer, rows_of(pos, me_d), :], own_sem.at[slot])

    for pos in range(count):
        rows, cols = shapes[pos]

        def body(layer, _, pos=pos, rows=rows, cols=cols):
            weight_copy(pos, layer).start()
            inbox_copy(pos, layer).start()
            if pos == 0:
                pl.when(layer >= SEND_SLOTS)(lambda: own_copy(pos, layer - SEND_SLOTS).wait())
            else:
                at_offset(pos, layer, -SEND_SLOTS, layers, count, lambda p, l: own_copy(p, l).wait())
            slot = lax.rem(pos * layers + layer, SEND_SLOTS)
            block, row = held.spot(pos, layer)
            wide = pl.ds(0, cols)

            def step(t, _):
                at, there = pl.ds(pl.multiple_of(t * 32, 32), 32), pl.ds(pl.multiple_of(row + t * 32, 32), 32)
                outbox[slot, at, wide] = held_ref[1, block, there, wide].astype(jnp.bfloat16)
                return 0

            lax.fori_loop(0, rows // 32, step, 0, unroll=2)
            own_copy(pos, layer).start()
            return 0

        lax.fori_loop(0, layers, body, 0)
    for layer in range(layers - SEND_SLOTS, layers):
        own_copy(count - 1, layer).wait()
    for pos in range(count):
        def drain(layer, _, pos=pos):
            weight_copy(pos, layer).wait()
            inbox_copy(pos, layer).wait()
            return 0

        lax.fori_loop(0, layers, drain, 0)


def solution(mesh):
    model_size, data_size = mesh.shape["model"], mesh.shape["data"]
    in_specs = []
    for col_split in COLUMN_SPLIT:
        in_specs.extend([grad_spec(col_split), state_spec(col_split), state_spec(col_split), state_spec(col_split)])
    out_specs = tuple([replica_spec(col_split) for col_split in COLUMN_SPLIT] + [state_spec(col_split) for col_split in COLUMN_SPLIT] * 3)
    hbm, vmem = pl.BlockSpec(memory_space=pltpu.HBM), pl.BlockSpec(memory_space=pltpu.VMEM)

    def in_hbm(values):
        return [pltpu.with_memory_space_constraint(value, pltpu.HBM) for value in values]

    def in_vmem(values):
        return [pltpu.with_memory_space_constraint(value, pltpu.VMEM) for value in values]

    def device_step(*arrays):
        grads, weights, firsts, seconds = (list(arrays[n::4]) for n in range(4))
        kinds = len(COLUMN_SPLIT)
        layers = weights[0].shape[0]
        units = kinds * layers
        shapes = [weight.shape[1:] for weight in weights]
        rows_max, cols_max = max(s[0] for s in shapes), max(s[1] for s in shapes)
        held_type = pltpu.VMEM((2, Resident(None, layers, [shapes[k] for k in ORDER]).slots, rows_max, cols_max), jnp.float32)
        state_hbm = [jax.ShapeDtypeStruct(weight.shape, jnp.float32) for weight in weights]
        sums = pltpu.VMEM((units, 8, 128), jnp.float32)
        devices = model_size * data_size
        dma = pltpu.SemaphoreType.DMA

        held, coef = pl.pallas_call(
            functools.partial(grad_kernel, (layers, shapes, model_size, data_size)),
            out_shape=[held_type, pltpu.VMEM((8, 128), jnp.float32)],
            in_specs=[hbm] * 8, out_specs=[vmem] * 2,
            scratch_shapes=[pltpu.VMEM(weight.shape, jnp.bfloat16) for weight in weights] + [
                pltpu.VMEM((STAGE_SLOTS, rows_max, cols_max), jnp.float32), pltpu.VMEM((SEND_SLOTS, rows_max, cols_max), jnp.bfloat16),
                pltpu.VMEM((8, 128), jnp.float32), pltpu.VMEM((devices, 8, 128), jnp.float32),
                dma((STAGE_SLOTS,)), dma((units,)), dma((units,)), dma((SEND_SLOTS,)), dma((units,)), dma((devices - 1,)), dma((devices,))],
            compiler_params=pltpu.CompilerParams(collective_id=0, has_side_effects=True, vmem_limit_bytes=SCOPED_BYTES),
            name="grad_mean",
        )(*in_hbm(grads + weights))

        outs = pl.pallas_call(
            functools.partial(adam_kernel, (layers, shapes)),
            out_shape=[held_type] + state_hbm + state_hbm + [sums, sums],
            in_specs=[vmem] * 2 + [hbm] * 8, out_specs=[vmem] + [hbm] * 8 + [vmem] * 2,
            input_output_aliases={1: 0},
            scratch_shapes=[pltpu.VMEM((STATE_SLOTS, 2, rows_max, cols_max), jnp.float32), dma((STATE_SLOTS, 2)), dma((STATE_SLOTS, 2))],
            compiler_params=pltpu.CompilerParams(vmem_limit_bytes=SCOPED_BYTES),
            name="adam",
        )(*in_vmem([coef, held]), *in_hbm(firsts + seconds))
        held, new_firsts, new_seconds, usq, wsq = outs[0], outs[1:5], outs[5:9], outs[9], outs[10]

        outs = pl.pallas_call(
            functools.partial(weight_kernel, (layers, shapes, model_size, data_size)),
            out_shape=[held_type] + [pltpu.VMEM(weight.shape, jnp.bfloat16) for weight in weights],
            in_specs=[vmem] * 3, out_specs=[vmem] * 5,
            input_output_aliases={2: 0},
            scratch_shapes=[pltpu.VMEM(held_type.shape[1:], jnp.bfloat16), pltpu.VMEM((devices, 8, 128), jnp.float32),
                            dma((devices - 1,)), dma((devices,)), dma((units,)), dma((units,))],
            compiler_params=pltpu.CompilerParams(collective_id=1, has_side_effects=True, vmem_limit_bytes=SCOPED_BYTES),
            name="new_weight",
        )(*in_vmem([usq, wsq, held]))

        outs = pl.pallas_call(
            functools.partial(write_kernel, (layers, shapes)),
            out_shape=state_hbm + [jax.ShapeDtypeStruct((layers, data_size * rows, cols), jnp.bfloat16) for rows, cols in shapes],
            in_specs=[vmem] * 5, out_specs=[hbm] * 8,
            scratch_shapes=[pltpu.VMEM((SEND_SLOTS, rows_max, cols_max), jnp.bfloat16), dma((units,)), dma((units,)), dma((SEND_SLOTS,))],
            compiler_params=pltpu.CompilerParams(vmem_limit_bytes=SCOPED_BYTES),
            name="write_out",
        )(*in_vmem(outs))
        return tuple(outs[4:]) + tuple(outs[:4]) + tuple(new_firsts) + tuple(new_seconds)

    return jax.shard_map(device_step, mesh=mesh, in_specs=tuple(in_specs), out_specs=out_specs, check_vma=False)
```

```python
import functools

import jax
import jax.numpy as jnp
from jax import lax
from jax.experimental import pallas as pl
from jax.experimental.pallas import tpu as pltpu
from jax.sharding import PartitionSpec as P

LEARN_RATE = 0.08
BETA_ONE = 0.9
BETA_TWO = 0.999
ADAM_EPS = 1e-6
DECAY_RATE = 0.01
MAX_NORM = 1.0
STEP_COUNT = 100
COLUMN_SPLIT = (True, False, True, False)
ORDER = (2, 3, 0, 1)
MESH_ID = pl.DeviceIdType.MESH
SCOPED_BYTES = 53 * 2**18

STAGE_SLOTS = 5
SEND_SLOTS = 6
COMBINE_LAG = 8
WEIGHT_AHEAD = 4
STATE_SLOTS = 12
STATE_AHEAD = 6
PACK_SLOTS = 12
STEP_ROWS = 32
TINY = 1.1754944e-38


def grad_spec(col_split):
    return P("data", None, None, "model") if col_split else P("data", None, "model", None)


def state_spec(col_split):
    return P(None, "data", "model") if col_split else P(None, ("model", "data"), None)


def replica_spec(col_split):
    return P(None, None, "model") if col_split else P(None, "model", None)


def at_offset(pos, idx, off, layers, count, action):
    target = idx + off
    if off == 0:
        action(pos, idx)
    elif off > 0:
        pl.when(target < layers)(lambda: action(pos, target))
        if pos + 1 < count:
            pl.when(target >= layers)(lambda: action(pos + 1, target - layers))
    else:
        pl.when(target >= 0)(lambda: action(pos, target))
        if pos > 0:
            pl.when(target < 0)(lambda: action(pos - 1, target + layers))


def fold_rows(block):
    return functools.reduce(jnp.add, [block[lo:lo + 8] for lo in range(0, block.shape[0], 8)])


def fold_lanes(acc):
    return functools.reduce(jnp.add, [acc[:, lo:lo + 128] for lo in range(0, acc.shape[1], 128)])


class Resident:
    def __init__(self, ref, layers, shapes):
        self.ref, self.shapes = ref, shapes
        full = max(rows for rows, _ in shapes)
        self.packed = [full // rows for rows, _ in shapes]
        self.base, total = [], 0
        for packed in self.packed:
            self.base.append(total)
            total += -(-layers // packed)
        self.slots = total

    def spot(self, pos, layer):
        packed = self.packed[pos]
        if packed == 1:
            return self.base[pos] + layer, 0
        rows = self.shapes[pos][0]
        return self.base[pos] + layer // packed, pl.multiple_of(lax.rem(layer, packed) * rows, rows)

    def block(self, which, pos, layer):
        return self.part(self.ref.at[which], pos, layer)

    def part(self, ref, pos, layer):
        rows, cols = self.shapes[pos]
        slot, row = self.spot(pos, layer)
        return ref.at[slot, pl.ds(row, rows), pl.ds(0, cols)]


def other_devices(model_size, data_size):
    return [(dm, dd) for dm in range(model_size) for dd in range(data_size) if (dm, dd) != (0, 0)]


class Peers:
    def __init__(self, model_size, data_size):
        self.model_size, self.data_size = model_size, data_size
        self.me_m, self.me_d = lax.axis_index("model"), lax.axis_index("data")
        self.me = self.me_m * data_size + self.me_d
        self.offsets = other_devices(model_size, data_size)

    def there(self, off):
        return lax.rem(self.me_m + off[0], self.model_size), lax.rem(self.me_d + off[1], self.data_size)

    def back(self, off):
        from_m = lax.rem(self.me_m + self.model_size - off[0], self.model_size)
        from_d = lax.rem(self.me_d + self.data_size - off[1], self.data_size)
        return from_m * self.data_size + from_d

    def arrive(self):
        barrier = pltpu.get_barrier_semaphore()
        for off in self.offsets:
            to_m, to_d = self.there(off)
            pl.semaphore_signal(barrier, inc=1, device_id=(to_m, to_d), device_id_type=MESH_ID)

    def await_all(self):
        pl.semaphore_wait(pltpu.get_barrier_semaphore(), len(self.offsets))

    def copies(self, slots, send_sem, recv_sem):
        out = []
        for num, off in enumerate(self.offsets):
            to_m, to_d = self.there(off)
            out.append(pltpu.make_async_remote_copy(
                src_ref=slots.at[self.me], dst_ref=slots.at[self.me], send_sem=send_sem.at[num],
                recv_sem=recv_sem.at[self.me], device_id=(to_m, to_d), device_id_type=MESH_ID))
        return out

    def wait_copies(self, copies, slots, send_sem, recv_sem):
        for num, off in enumerate(self.offsets):
            src = self.back(off)
            copies[num].wait_send()
            to_m, to_d = self.there(off)
            pltpu.make_async_remote_copy(
                src_ref=slots.at[src], dst_ref=slots.at[src], send_sem=send_sem.at[num],
                recv_sem=recv_sem.at[src], device_id=(to_m, to_d), device_id_type=MESH_ID).wait_recv()


def grad_kernel(dims, g0, g1, g2, g3, w0, w1, w2, w3, held_ref, coef_ref,
                r0, r1, r2, r3, stage, outbox, acc_ref, slots, other_sem, own_sem, w_sem, send_sem, recv_sem, tile_send, tile_recv):
    layers, shapes, model_size, data_size = dims
    grads, weights = [(g0, g1, g2, g3)[k] for k in ORDER], [(w0, w1, w2, w3)[k] for k in ORDER]
    inbox, shapes = [(r0, r1, r2, r3)[k] for k in ORDER], [shapes[k] for k in ORDER]
    count = len(ORDER)
    held = Resident(held_ref, layers, shapes)
    peers = Peers(model_size, data_size)
    mine, theirs = peers.me_d, 1 - peers.me_d
    peers.arrive()

    def number(pos, layer):
        return pos * layers + layer

    def rows_of(pos, who):
        return pl.ds(pl.multiple_of(who * shapes[pos][0], shapes[pos][0]), shapes[pos][0])

    def load_other(pos, layer):
        rows, cols = shapes[pos]
        slot = lax.rem(number(pos, layer), STAGE_SLOTS)
        return pltpu.make_async_copy(grads[pos].at[0, layer, rows_of(pos, theirs), :], stage.at[slot, pl.ds(0, rows), pl.ds(0, cols)], other_sem.at[slot])

    def load_own(pos, layer):
        return pltpu.make_async_copy(grads[pos].at[0, layer, rows_of(pos, mine), :], held.block(0, pos, layer), own_sem.at[number(pos, layer)])

    def load_weight(pos, layer):
        return pltpu.make_async_copy(weights[pos].at[layer], held.block(1, pos, layer), w_sem.at[number(pos, layer)])

    def send(pos, layer):
        rows, cols = shapes[pos]
        slot = lax.rem(number(pos, layer), SEND_SLOTS)
        return pltpu.make_async_remote_copy(
            src_ref=outbox.at[slot, pl.ds(0, rows), pl.ds(0, cols)], dst_ref=inbox[pos].at[layer], send_sem=send_sem.at[slot],
            recv_sem=recv_sem.at[number(pos, layer)], device_id=(peers.me_m, theirs), device_id_type=MESH_ID)

    def pack(pos, layer):
        rows, cols = shapes[pos]
        num = number(pos, layer)
        slot, box = lax.rem(num, STAGE_SLOTS), lax.rem(num, SEND_SLOTS)
        load_other(pos, layer).wait()

        def step(t, _):
            at = pl.ds(pl.multiple_of(t * 32, 32), 32)
            outbox[box, at, pl.ds(0, cols)] = stage[slot, at, pl.ds(0, cols)].astype(jnp.bfloat16)
            return 0

        lax.fori_loop(0, rows // 32, step, 0, unroll=2)

    def combine(pos, layer):
        rows, cols = shapes[pos]
        load_own(pos, layer).wait()
        send(pos, layer).wait_recv()
        block, row = held.spot(pos, layer)
        wide = pl.ds(0, cols)

        def step(t, acc):
            at = pl.ds(pl.multiple_of(t * 32, 32), 32)
            there = pl.ds(pl.multiple_of(row + t * 32, 32), 32)
            own = held_ref[0, block, there, wide].astype(jnp.bfloat16).astype(jnp.float32)
            mean = (own + inbox[pos][layer, at, :].astype(jnp.float32)) * (1.0 / data_size)
            held_ref[0, block, there, wide] = mean
            return acc + fold_rows(mean * mean)

        acc = lax.fori_loop(0, rows // 32, step, jnp.zeros((8, cols), jnp.float32))
        acc_ref[...] += fold_lanes(acc)

    acc_ref[...] = jnp.zeros_like(acc_ref)
    for layer in range(STAGE_SLOTS):
        load_other(0, layer).start()
        load_own(0, layer).start()
    for layer in range(WEIGHT_AHEAD):
        load_weight(0, layer).start()
    for pos in range(count):
        def body(layer, _, pos=pos):
            if pos == 0:
                pl.when(layer >= SEND_SLOTS)(lambda: send(pos, layer - SEND_SLOTS).wait_send())
            else:
                at_offset(pos, layer, -SEND_SLOTS, layers, count, lambda p, l: send(p, l).wait_send())
            pack(pos, layer)
            if pos == 0:
                pl.when(layer == 0)(peers.await_all)
            at_offset(pos, layer, -1, layers, count, lambda p, l: send(p, l).start())

            def ahead(p, l):
                load_other(p, l).start()
                load_own(p, l).start()

            at_offset(pos, layer, STAGE_SLOTS, layers, count, ahead)
            at_offset(pos, layer, WEIGHT_AHEAD, layers, count, lambda p, l: load_weight(p, l).start())
            at_offset(pos, layer, -COMBINE_LAG, layers, count, combine)
            return 0

        lax.fori_loop(0, layers, body, 0)
    last = count - 1
    send(last, layers - 1).start()

    def finish(layer, _):
        combine(last, layer)
        return 0

    lax.fori_loop(layers - COMBINE_LAG, layers, finish, 0)
    for layer in range(layers - SEND_SLOTS, layers):
        send(last, layer).wait_send()

    slots[peers.me] = acc_ref[...]
    copies = peers.copies(slots, tile_send, tile_recv)
    for copy in copies:
        copy.start()
    for pos in range(count):
        def drain(layer, _, pos=pos):
            load_weight(pos, layer).wait()
            return 0

        lax.fori_loop(0, layers, drain, 0)
    peers.wait_copies(copies, slots, tile_send, tile_recv)
    total = functools.reduce(jnp.add, [slots[n] for n in range(model_size * data_size)])
    total = jnp.sum(jnp.sum(total, axis=1, keepdims=True), axis=0, keepdims=True)
    coef_ref[...] = jnp.broadcast_to(jnp.minimum(1.0, MAX_NORM / jnp.sqrt(total)), coef_ref.shape)


def adam_kernel(dims, *refs):
    layers, shapes = dims
    count = len(ORDER)
    coef_ref = refs[0]
    m_in, v_in, held_ref, m_out, v_out = refs[2:6], refs[6:10], refs[10], refs[11:15], refs[15:19]
    usq_ref, wsq_ref, ring, load_sem, store_sem = refs[19:]
    pick = lambda group: [group[k] for k in ORDER]
    m_in, v_in, m_out, v_out, shapes = map(pick, (m_in, v_in, m_out, v_out, shapes))
    held = Resident(held_ref, layers, shapes)
    coef = jnp.max(coef_ref[...])
    first_scale, second_scale = (1.0 - BETA_ONE) * coef, (1.0 - BETA_TWO) ** 0.5 * coef
    first_fix = 1.0 - BETA_ONE ** STEP_COUNT
    root_scale, eps_scale = first_fix / (1.0 - BETA_TWO ** STEP_COUNT) ** 0.5, first_fix * ADAM_EPS

    def number(pos, layer):
        return pos * layers + layer

    def window(pos, slot, which):
        rows, cols = shapes[pos]
        return ring.at[slot, which, pl.ds(0, rows), pl.ds(0, cols)]

    def loads(pos, layer):
        slot = lax.rem(number(pos, layer), STATE_SLOTS)
        return [pltpu.make_async_copy(src[pos].at[layer], window(pos, slot, which), load_sem.at[slot, which]) for which, src in enumerate((m_in, v_in))]

    def stores(pos, layer):
        slot = lax.rem(number(pos, layer), STATE_SLOTS)
        return [pltpu.make_async_copy(window(pos, slot, which), dst[pos].at[layer], store_sem.at[slot, which]) for which, dst in enumerate((m_out, v_out))]

    def start_loads(pos, layer):
        for copy in loads(pos, layer):
            copy.start()

    def wait_stores(pos, layer):
        for copy in stores(pos, layer):
            copy.wait()

    def compute(pos, layer):
        rows, cols = shapes[pos]
        num = number(pos, layer)
        slot = lax.rem(num, STATE_SLOTS)
        block, row = held.spot(pos, layer)

        def step(t, accs):
            at, wide = pl.ds(pl.multiple_of(t * STEP_ROWS, STEP_ROWS), STEP_ROWS), pl.ds(0, cols)
            there = pl.ds(pl.multiple_of(row + t * STEP_ROWS, STEP_ROWS), STEP_ROWS)
            mean, weight = held_ref[0, block, there, wide], held_ref[1, block, there, wide]
            first = BETA_ONE * ring[slot, 0, at, wide] + first_scale * mean
            scaled = second_scale * mean
            second = BETA_TWO * ring[slot, 1, at, wide] + scaled * scaled
            root = second * lax.rsqrt(jnp.maximum(second, TINY))
            update = first / (root * root_scale + eps_scale) + DECAY_RATE * weight
            ring[slot, 0, at, wide] = first
            ring[slot, 1, at, wide] = second
            held_ref[0, block, there, wide] = update
            return accs[0] + fold_rows(update * update), accs[1] + fold_rows(weight * weight)

        zero = jnp.zeros((8, cols), jnp.float32)
        usq, wsq = lax.fori_loop(0, rows // STEP_ROWS, step, (zero, zero))
        usq_ref[num] = fold_lanes(usq)
        wsq_ref[num] = fold_lanes(wsq)

    for layer in range(STATE_AHEAD):
        start_loads(0, layer)
    for pos in range(count):
        def body(layer, _, pos=pos):
            at_offset(pos, layer, STATE_AHEAD - STATE_SLOTS, layers, count, wait_stores)
            at_offset(pos, layer, STATE_AHEAD, layers, count, start_loads)
            for copy in loads(pos, layer):
                copy.wait()
            compute(pos, layer)
            for copy in stores(pos, layer):
                copy.start()
            return 0

        lax.fori_loop(0, layers, body, 0)
    for layer in range(layers - STATE_SLOTS + STATE_AHEAD, layers):
        wait_stores(count - 1, layer)


def weight_kernel(dims, usq_ref, wsq_ref, _, held_ref, inbox, outbox, slots, tile_send, tile_recv, send_sem, recv_sem):
    layers, shapes, model_size, data_size = dims
    count = len(ORDER)
    shapes = [shapes[k] for k in ORDER]
    held = Resident(held_ref, layers, shapes)
    peers = Peers(model_size, data_size)
    peers.arrive()

    def number(pos, layer):
        return pos * layers + layer

    def send(pos, layer):
        return pltpu.make_async_remote_copy(
            src_ref=held.part(outbox, pos, layer), dst_ref=held.part(inbox, pos, layer), send_sem=send_sem.at[number(pos, layer)],
            recv_sem=recv_sem.at[number(pos, layer)], device_id=(peers.me_m, 1 - peers.me_d), device_id_type=MESH_ID)

    def by_lane(ref):
        part = jnp.sum(ref[...], axis=1)
        part = jnp.concatenate([part, jnp.zeros((128 - part.shape[0], 128), jnp.float32)], axis=0)
        return jnp.sum(part.T, axis=0, keepdims=True)

    row = lax.broadcasted_iota(jnp.int32, (8, 128), 0)
    lane = lax.broadcasted_iota(jnp.int32, (8, 128), 1)
    slots[peers.me] = jnp.where(row == 0, by_lane(usq_ref), by_lane(wsq_ref))
    peers.await_all()
    copies = peers.copies(slots, tile_send, tile_recv)
    for copy in copies:
        copy.start()
    peers.wait_copies(copies, slots, tile_send, tile_recv)
    total = functools.reduce(jnp.add, [slots[n] for n in range(model_size * data_size)])
    root = jnp.sqrt(total)
    live = (row == 1) & (lane < count * layers)
    rates = jnp.where(live, LEARN_RATE * (root / jnp.where(lane < count * layers, root[0:1], 1.0)), 0.0)

    for pos in range(count):
        rows, cols = shapes[pos]

        def body(layer, _, pos=pos, rows=rows, cols=cols):
            num = number(pos, layer)
            rate = jnp.sum(jnp.where(lane == num, rates, 0.0))
            block, row = held.spot(pos, layer)
            wide = pl.ds(0, cols)

            def step(t, _):
                there = pl.ds(pl.multiple_of(row + t * 16, 16), 16)
                new = held_ref[1, block, there, wide] - rate * held_ref[0, block, there, wide]
                held_ref[1, block, there, wide] = new
                outbox[block, there, wide] = new.astype(jnp.bfloat16)
                return 0

            lax.fori_loop(0, rows // 16, step, 0, unroll=2)
            at_offset(pos, layer, -1, layers, count, lambda p, l: send(p, l).start())
            return 0

        lax.fori_loop(0, layers, body, 0)
    send(count - 1, layers - 1).start()
    for pos in range(count):
        def drain(layer, _, pos=pos):
            send(pos, layer).wait()
            return 0

        lax.fori_loop(0, layers, drain, 0)


def write_kernel(dims, held_ref, inbox, w0, w1, w2, w3, r0, r1, r2, r3, outbox, weight_sem, inbox_sem, own_sem):
    layers, shapes = dims
    count = len(ORDER)
    pick = lambda group: [group[k] for k in ORDER]
    weights, replicas, shapes = map(pick, ((w0, w1, w2, w3), (r0, r1, r2, r3), shapes))
    held = Resident(held_ref, layers, shapes)
    me_d = lax.axis_index("data")

    def rows_of(pos, who):
        return pl.ds(pl.multiple_of(who * shapes[pos][0], shapes[pos][0]), shapes[pos][0])

    def weight_copy(pos, layer):
        return pltpu.make_async_copy(held.block(1, pos, layer), weights[pos].at[layer], weight_sem.at[pos * layers + layer])

    def inbox_copy(pos, layer):
        return pltpu.make_async_copy(held.part(inbox, pos, layer), replicas[pos].at[layer, rows_of(pos, 1 - me_d), :], inbox_sem.at[pos * layers + layer])

    def own_copy(pos, layer):
        rows, cols = shapes[pos]
        slot = lax.rem(pos * layers + layer, PACK_SLOTS)
        return pltpu.make_async_copy(outbox.at[slot, pl.ds(0, rows), pl.ds(0, cols)], replicas[pos].at[layer, rows_of(pos, me_d), :], own_sem.at[slot])

    for pos in range(count):
        def issue(layer, _, pos=pos):
            weight_copy(pos, layer).start()
            inbox_copy(pos, layer).start()
            return 0

        lax.fori_loop(0, layers, issue, 0)
    for pos in range(count):
        rows, cols = shapes[pos]

        def body(layer, _, pos=pos, rows=rows, cols=cols):
            if pos == 0:
                pl.when(layer >= PACK_SLOTS)(lambda: own_copy(pos, layer - PACK_SLOTS).wait())
            else:
                at_offset(pos, layer, -PACK_SLOTS, layers, count, lambda p, l: own_copy(p, l).wait())
            slot = lax.rem(pos * layers + layer, PACK_SLOTS)
            block, row = held.spot(pos, layer)
            wide = pl.ds(0, cols)

            def step(t, _):
                at, there = pl.ds(pl.multiple_of(t * 32, 32), 32), pl.ds(pl.multiple_of(row + t * 32, 32), 32)
                outbox[slot, at, wide] = held_ref[1, block, there, wide].astype(jnp.bfloat16)
                return 0

            lax.fori_loop(0, rows // 32, step, 0, unroll=2)
            own_copy(pos, layer).start()
            return 0

        lax.fori_loop(0, layers, body, 0)
    for layer in range(layers - PACK_SLOTS, layers):
        own_copy(count - 1, layer).wait()
    for pos in range(count):
        def drain(layer, _, pos=pos):
            weight_copy(pos, layer).wait()
            inbox_copy(pos, layer).wait()
            return 0

        lax.fori_loop(0, layers, drain, 0)


def solution(mesh):
    model_size, data_size = mesh.shape["model"], mesh.shape["data"]
    in_specs = []
    for col_split in COLUMN_SPLIT:
        in_specs.extend([grad_spec(col_split), state_spec(col_split), state_spec(col_split), state_spec(col_split)])
    out_specs = tuple([replica_spec(col_split) for col_split in COLUMN_SPLIT] + [state_spec(col_split) for col_split in COLUMN_SPLIT] * 3)
    hbm, vmem = pl.BlockSpec(memory_space=pltpu.HBM), pl.BlockSpec(memory_space=pltpu.VMEM)

    def in_hbm(values):
        return [pltpu.with_memory_space_constraint(value, pltpu.HBM) for value in values]

    def in_vmem(values):
        return [pltpu.with_memory_space_constraint(value, pltpu.VMEM) for value in values]

    def device_step(*arrays):
        grads, weights, firsts, seconds = (list(arrays[n::4]) for n in range(4))
        kinds = len(COLUMN_SPLIT)
        layers = weights[0].shape[0]
        units = kinds * layers
        shapes = [weight.shape[1:] for weight in weights]
        rows_max, cols_max = max(s[0] for s in shapes), max(s[1] for s in shapes)
        held_type = pltpu.VMEM((2, Resident(None, layers, [shapes[k] for k in ORDER]).slots, rows_max, cols_max), jnp.float32)
        state_hbm = [jax.ShapeDtypeStruct(weight.shape, jnp.float32) for weight in weights]
        sums = pltpu.VMEM((units, 8, 128), jnp.float32)
        devices = model_size * data_size
        dma = pltpu.SemaphoreType.DMA

        held, coef = pl.pallas_call(
            functools.partial(grad_kernel, (layers, shapes, model_size, data_size)),
            out_shape=[held_type, pltpu.VMEM((8, 128), jnp.float32)],
            in_specs=[hbm] * 8, out_specs=[vmem] * 2,
            scratch_shapes=[pltpu.VMEM(weight.shape, jnp.bfloat16) for weight in weights] + [
                pltpu.VMEM((STAGE_SLOTS, rows_max, cols_max), jnp.float32), pltpu.VMEM((SEND_SLOTS, rows_max, cols_max), jnp.bfloat16),
                pltpu.VMEM((8, 128), jnp.float32), pltpu.VMEM((devices, 8, 128), jnp.float32),
                dma((STAGE_SLOTS,)), dma((units,)), dma((units,)), dma((SEND_SLOTS,)), dma((units,)), dma((devices - 1,)), dma((devices,))],
            compiler_params=pltpu.CompilerParams(collective_id=0, has_side_effects=True, vmem_limit_bytes=SCOPED_BYTES),
            name="grad_mean",
        )(*in_hbm(grads + weights))

        outs = pl.pallas_call(
            functools.partial(adam_kernel, (layers, shapes)),
            out_shape=[held_type] + state_hbm + state_hbm + [sums, sums],
            in_specs=[vmem] * 2 + [hbm] * 8, out_specs=[vmem] + [hbm] * 8 + [vmem] * 2,
            input_output_aliases={1: 0},
            scratch_shapes=[pltpu.VMEM((STATE_SLOTS, 2, rows_max, cols_max), jnp.float32), dma((STATE_SLOTS, 2)), dma((STATE_SLOTS, 2))],
            compiler_params=pltpu.CompilerParams(vmem_limit_bytes=SCOPED_BYTES),
            name="adam",
        )(*in_vmem([coef, held]), *in_hbm(firsts + seconds))
        held, new_firsts, new_seconds, usq, wsq = outs[0], outs[1:5], outs[5:9], outs[9], outs[10]

        outs = pl.pallas_call(
            functools.partial(weight_kernel, (layers, shapes, model_size, data_size)),
            out_shape=[held_type, pltpu.VMEM(held_type.shape[1:], jnp.bfloat16)],
            in_specs=[vmem] * 3, out_specs=[vmem] * 2,
            input_output_aliases={2: 0},
            scratch_shapes=[pltpu.VMEM(held_type.shape[1:], jnp.bfloat16), pltpu.VMEM((devices, 8, 128), jnp.float32),
                            dma((devices - 1,)), dma((devices,)), dma((units,)), dma((units,))],
            compiler_params=pltpu.CompilerParams(collective_id=1, has_side_effects=True, vmem_limit_bytes=SCOPED_BYTES),
            name="new_weight",
        )(*in_vmem([usq, wsq, held]))

        outs = pl.pallas_call(
            functools.partial(write_kernel, (layers, shapes)),
            out_shape=state_hbm + [jax.ShapeDtypeStruct((layers, data_size * rows, cols), jnp.bfloat16) for rows, cols in shapes],
            in_specs=[vmem] * 2, out_specs=[hbm] * 8,
            scratch_shapes=[pltpu.VMEM((PACK_SLOTS, rows_max, cols_max), jnp.bfloat16), dma((units,)), dma((units,)), dma((PACK_SLOTS,))],
            compiler_params=pltpu.CompilerParams(vmem_limit_bytes=SCOPED_BYTES),
            name="write_out",
        )(*in_vmem(outs))
        return tuple(outs[4:]) + tuple(outs[:4]) + tuple(new_firsts) + tuple(new_seconds)

    return jax.shard_map(device_step, mesh=mesh, in_specs=tuple(in_specs), out_specs=out_specs, check_vma=False)
```
